32 devices in a mesh: gx: 32 (over z, y, x, core).
Axes of the slice: x: 2, y: 2, z: 4, core: 2. Of those that a mesh axis runs over, the one named last changes fastest.
Arguments:
- populations0: float32 [27, 32, 2048], P(None, 'gx'), as said below
- force: float32 [3, 32, 2048], P(None, 'gx'), may hold values from -0.05 to 0.05
- solid: int32 [32, 2048], P('gx'), may hold values 0 or 1
- newton_count: int32 [32, 2048], P('gx'), may hold values from 1 to 3
- cotangent: float32 [27, 32, 2048], P(None, 'gx'), may hold values from -6 to 6
Outputs:
- final_ratio: float32 [27, 32, 2048], P(None, 'gx')
- grad_populations: float32 [27, 32, 2048], P(None, 'gx')
- grad_force: float32 [3, 32, 2048], P(None, 'gx')
The draws below stay inside these ranges and needn't reach their ends.
Inputs may be any that keep to these rules, and one draw needn't show every extreme that they name: `populations0`: every population lies between 0.6 and 1.4 times its lattice weight.
All inputs are finite; a program needn't handle non-finite values. No bound on the sum of `solid` on one device may be relied on, other than what follows from the above.
Results may differ from the reference program's by a relative error of at most 0.0003.
Values sent between devices are 32-bit elements; how exact they have to be, the bound alone decides.
No kernel may reach another device: no remote copies, remote signals or barrier semaphores. Data moves between devices by JAX's collectives and lax.ppermute only.
A program may use at most 64 MiB of HBM per device.

```python
import jax
import jax.numpy as jnp
import numpy as np
from jax import lax

NY = 16
NZ = 128
STEPS = 4
NEWTON = 3
NX = 32
NYZ = 2048


def draw_populations0(key, part):
    speeds_table = np.array([[a, b, c] for a in (-1, 0, 1) for b in (-1, 0, 1) for c in (-1, 0, 1)])
    levels = np.abs(speeds_table).sum(axis=1)
    weight_table = np.array([8.0 / 27.0, 2.0 / 27.0, 1.0 / 54.0, 1.0 / 216.0])[levels]
    weight = jnp.asarray(weight_table, jnp.float32)[:, None, None]
    shape = (27, NX, NY * NZ)
    ratio = 1.0 + 0.15 * jnp.clip(jax.random.normal(key, shape, jnp.float32), -2.5, 2.5)
    return weight * ratio


def with_ends(values, stream_key, low, high):
    longest = values.shape.index(max(values.shape))
    spots = []
    for shift in (0, 1):
        where = [jax.random.randint(jax.random.fold_in(stream_key, axis), (), 0, length) for axis, length in enumerate(values.shape)]
        where[longest] = (where[longest] + shift) % values.shape[longest]
        spots.append(tuple(where))
    return values.at[spots[0]].set(low).at[spots[1]].set(high)


def block_scale(stream_key, dims, cuts, least, top_value):
    def one(axis_at, shards_of):
        heights = jax.random.uniform(jax.random.fold_in(jax.random.fold_in(stream_key, 6), axis_at), (shards_of,), jnp.float32, least / len(cuts), top_value / len(cuts))
        return jnp.repeat(jnp.exp(heights), dims[axis_at] // shards_of).reshape((-1,) + (1,) * (len(dims) - axis_at - 1))

    level = one(*cuts[0])
    for cut in cuts[1:]:
        level = level * one(*cut)
    return level


def bell_draw(key, shape, width, bound, cuts=(), kind=jnp.bfloat16):
    drawn = width * jax.random.normal(key, shape, jnp.float32)
    if cuts:
        drawn = drawn * block_scale(key, shape, cuts, -0.22, 0.18)
    return jnp.clip(drawn, -bound, bound).astype(kind)


def setup_inputs(seed: int = 0) -> dict:
    streams_of = jax.random.split(jax.random.key(seed), 6)
    return {
        "populations0": draw_populations0(jax.random.fold_in(streams_of[5], 71), 0),
        "force": jnp.clip(jax.random.uniform(streams_of[1], (3, NX, NYZ), jnp.float32, -0.05, 0.05) * block_scale(streams_of[1], (3, NX, NYZ), ((1, 32),), -0.4, 0.0), -0.05, 0.05),
        "solid": with_ends((jax.random.randint(streams_of[2], (NX, NYZ), 0, 8) < 1).astype(jnp.int32), jax.random.fold_in(streams_of[2], 1), 0, 1),
        "newton_count": with_ends(jax.random.randint(streams_of[3], (NX, NYZ), 1, NEWTON + 1), jax.random.fold_in(streams_of[3], 1), 1, NEWTON).astype(jnp.int32),
        "cotangent": bell_draw(streams_of[4], (27, NX, NYZ), 1.0, 6.0, ((1, 32),), jnp.float32),
    }


BETA = 0.85

def tables():
    speeds_table = np.array([[a, b, c] for a in (-1, 0, 1) for b in (-1, 0, 1) for c in (-1, 0, 1)])
    levels = np.abs(speeds_table).sum(axis=1)
    weight_table = np.array([8.0 / 27.0, 2.0 / 27.0, 1.0 / 54.0, 1.0 / 216.0])[levels]
    return (speeds_table, weight_table)

def collide(populations, force, solid, newton_count):
    speeds_table, weight_table = tables()
    velocity = jnp.asarray(speeds_table, jnp.float32)
    weight = jnp.asarray(weight_table, jnp.float32)[:, None, None]
    density = lax.optimization_barrier(jnp.sum(populations, axis=0))
    momentum = jnp.einsum('iq,ixs->qxs', velocity, populations, precision=lax.Precision.HIGHEST)
    bulk_velocity = (momentum + force) / density
    projected = jnp.einsum('iq,qxs->ixs', velocity, bulk_velocity, precision=lax.Precision.HIGHEST)
    squared_speed = lax.optimization_barrier(jnp.sum(bulk_velocity * bulk_velocity, axis=0))
    balance = weight * density * (1.0 + 3.0 * projected + 4.5 * projected * projected - 1.5 * squared_speed)
    offset = balance - populations
    entropy = lax.optimization_barrier(jnp.sum(populations * jnp.log(populations / weight), axis=0))
    reaches = jnp.where(offset < 0.0, populations / jnp.maximum(-offset, 0.001 * weight), 1000000000.0)
    ceiling = jnp.clip(0.9 * lax.optimization_barrier(jnp.min(reaches, axis=0)), 1.0, 2.0)
    factor = ceiling
    for iteration in range(NEWTON):
        blended = populations + factor * offset
        logged = jnp.log(blended / weight)
        excess = lax.optimization_barrier(jnp.sum(blended * logged, axis=0)) - entropy
        derivative = lax.optimization_barrier(jnp.sum(offset * (logged + 1.0), axis=0))
        bending = lax.optimization_barrier(jnp.sum(offset * offset / blended, axis=0))
        update = jnp.clip(factor - excess / jnp.maximum(derivative, 0.5 * bending), 1.0, ceiling)
        factor = jnp.where(newton_count > iteration, update, factor)
    factor = lax.stop_gradient(factor)
    relaxed = populations + BETA * factor * offset
    return jnp.where(solid[None] == 1, populations[::-1], relaxed)

def stream(post):
    speeds_table, weight_table = tables()
    lattice = post.reshape(27, NX, NY, NZ)
    shifted = [jnp.roll(lattice[number], tuple((int(v) for v in speeds_table[number])), axis=(0, 1, 2)) for number in range(27)]
    return jnp.stack(shifted).reshape(27, NX, NY * NZ)

def reference(populations0, force, solid, newton_count, cotangent):

    def rollout(start, pushed):
        state = start
        for section in range(STEPS):
            state = stream(collide(state, pushed, solid, newton_count))
        return state
    final, pullback = jax.vjp(rollout, populations0, force)
    grad_start, grad_push = pullback(cotangent)
    speeds_table, weight_table = tables()
    weight = jnp.asarray(weight_table, jnp.float32)[:, None, None]
    return (final / weight, grad_start, grad_push)
```

```python
import functools

import jax
import jax.numpy as jnp
from jax import lax
from jax.experimental import pallas as pl
from jax.experimental.pallas import tpu as pltpu
from jax.sharding import PartitionSpec as P

NZ = 128
NEWTON = 3
BETA = 0.85
AXIS = "gx"

OUT, MID, IN = 0, 1, 2
SCALE = 1.0 / 216.0
LEVELS = (216.0 * 8.0 / 27.0, 216.0 * 2.0 / 27.0, 216.0 / 54.0, 1.0)


def level(a, b, c):
    return abs(a - 1) + abs(b - 1) + abs(c - 1)


CLASSES = [[(a, b, c) for a in range(3) for b in range(3) for c in range(3) if level(a, b, c) == n] for n in range(4)]
EVERY = [d for group in CLASSES for d in group]


def slot(d):
    return d[0] * 9 + d[1] * 3 + d[2]


def opposite(d):
    return (2 - d[0], 2 - d[1], 2 - d[2])


def moved(x, b, c, sign):
    shift_y, shift_z = (sign * (b - 1)) % x.shape[0], (sign * (c - 1)) % x.shape[1]
    if shift_y:
        x = pltpu.roll(x, shift_y, 0)
    if shift_z:
        x = pltpu.roll(x, shift_z, 1)
    return x


def odd_device():
    return lax.rem(lax.axis_index(AXIS), 2)


def facing(odd):
    return 1.0 - 2.0 * odd.astype(jnp.float32)


def block_of(a, odd):
    return (a + odd * (2 - 2 * a)) * 9


def moments(get, second):
    along = []
    for a in range(3):
        rows = []
        for b in range(3):
            low, zero, high = get((a, b, 0)), get((a, b, 1)), get((a, b, 2))
            both = low + high
            rows.append((4.0 * zero + both, high - low, both))
        (l0, l1, l2), (z0, z1, z2), (h0, h1, h2) = rows
        edge = l0 + h0
        parts = [4.0 * z0 + edge, h0 - l0, 4.0 * z1 + (l1 + h1)]
        if second:
            parts += [edge, h1 - l1, 4.0 * z2 + (l2 + h2)]
        along.append(parts)
    low, zero, high = along

    def even(n):
        return 4.0 * zero[n] + (low[n] + high[n])

    result = [even(0), high[0] - low[0], even(1), even(2)]
    if second:
        result += [low[0] + high[0], even(3), even(5), high[1] - low[1], high[2] - low[2], even(4)]
    return result


def weighted(term):
    totals = None
    for group, weight in zip(CLASSES, LEVELS):
        sums = None
        for d in group:
            values = term(d)
            sums = list(values) if sums is None else [s + v for s, v in zip(sums, values)]
        sums = [weight * s for s in sums]
        totals = sums if totals is None else [t + s for t, s in zip(totals, sums)]
    return totals


def collide(get, force, solid, newton, offset, emit):
    mass, mx, my, mz = moments(get, False)
    density = SCALE * mass
    ux = (SCALE * mx + force[0]) / density
    uy = (SCALE * my + force[1]) / density
    uz = (SCALE * mz + force[2]) / density
    base = density * (1.0 - 1.5 * (ux * ux + uy * uy + uz * uz))
    linear, square = 3.0 * density, 4.5 * density
    projected = {}
    for d in EVERY:
        if d == (1, 1, 1) or opposite(d) in projected:
            continue
        total = None
        for speed, u in zip(d, (ux, uy, uz)):
            if speed == 1:
                continue
            if total is None:
                total, flip = u, speed
            else:
                total = total + u if speed == flip else total - u
        projected[d] = None
        even = base + square * total * total
        tilt = linear * total
        up, down = (d, opposite(d)) if flip == 2 else (opposite(d), d)
        offset[slot(up)] = (even + tilt) - get(up)
        offset[slot(down)] = (even - tilt) - get(down)
    offset[slot((1, 1, 1))] = base - get((1, 1, 1))

    reach = None

    def first(d):
        nonlocal reach
        value, step = get(d), offset[slot(d)]
        limit = jnp.where(step < 0.0, value / jnp.maximum(-step, 0.001), 1000000000.0)
        reach = limit if reach is None else jnp.minimum(reach, limit)
        return value * jnp.log(value), step

    entropy, drift = weighted(first)
    cap = jnp.clip(0.9 * reach, 1.0, 2.0)
    factor = cap
    for k in range(NEWTON):

        def term(d, factor=factor):
            step = offset[slot(d)]
            mixed = get(d) + factor * step
            logged = jnp.log(mixed)
            return mixed * logged, step * logged, step * step / mixed

        mixing, slope, bend = weighted(term)
        update = factor - (mixing - entropy) / jnp.maximum(slope + drift, 0.5 * bend)
        factor = jnp.where(newton > k, jnp.clip(update, 1.0, cap), factor)
    rate = BETA * factor
    for d in EVERY:
        emit(d, lambda d=d: jnp.where(solid == 1, get(opposite(d)), get(d) + rate * offset[slot(d)]))
    return ux, uy, uz, jnp.where(solid == 1, 0.0, rate)


def pull_back(get, saved, solid, emit):
    ux, uy, uz, rate = saved
    total, vx, vy, vz, txx, tyy, tzz, txy, txz, tyz = [SCALE * m for m in moments(get, True)]
    sx = txx * ux + txy * uy + txz * uz
    sy = txy * ux + tyy * uy + tyz * uz
    sz = txz * ux + tyz * uy + tzz * uz
    hx = 3.0 * vx + 9.0 * sx - 3.0 * ux * total
    hy = 3.0 * vy + 9.0 * sy - 3.0 * uy * total
    hz = 3.0 * vz + 9.0 * sz - 3.0 * uz * total
    grown = (
        total * (1.0 - 1.5 * (ux * ux + uy * uy + uz * uz))
        + 3.0 * (vx * ux + vy * uy + vz * uz)
        + 4.5 * (sx * ux + sy * uy + sz * uz)
    )
    px, py, pz = rate * hx, rate * hy, rate * hz
    kept = rate * (grown - (hx * ux + hy * uy + hz * uz))
    stay = 1.0 - rate
    for a in range(3):
        at_a = kept + (a - 1) * px if a != 1 else kept
        for b in range(3):
            at_b = at_a + (b - 1) * py if b != 1 else at_a
            for c in range(3):
                d = (a, b, c)
                shared = at_b + (c - 1) * pz if c != 1 else at_b
                emit(d, lambda d=d, shared=shared: jnp.where(solid == 1, get(opposite(d)), stay * get(d) + shared))
    return px, py, pz


def reader(*blocks):
    def get(d):
        ref, start = blocks[d[0]]
        return ref[start + d[1] * 3 + d[2]]

    return get


def writer(sign, **targets):
    table = {OUT: targets.get("out"), MID: targets.get("mid"), IN: targets.get("into")}

    def emit(d, value):
        if table[d[0]] is None:
            return
        ref, start = table[d[0]]
        ref[start + d[1] * 3 + d[2]] = moved(value(), d[1], d[2], sign)

    return emit


def keep(ref, values):
    for n, value in enumerate(values):
        ref[n] = value


def saved_of(ref):
    return tuple(ref[n] for n in range(4))


def framed(force, at=0):
    return facing(odd_device()) * force[at], force[at + 1], force[at + 2]


def first_kernel(start, force, solid, newton, inward, outward, saved, scaled, offset):
    odd = odd_device()
    for d in EVERY:
        scaled[slot(d)] = (216.0 / LEVELS[level(*d)]) * start[block_of(d[0], odd) + d[1] * 3 + d[2]]
    get = reader((scaled, 0), (scaled, 9), (scaled, 18))
    keep(saved, collide(get, framed(force), solid[...], newton[...], offset, writer(1, into=(inward, 0), out=(outward, 0), mid=(outward, 9))))
    for n in range(3):
        outward[18 + n] = force[n]
    outward[21] = solid[...].astype(jnp.float32)
    outward[22] = newton[...].astype(jnp.float32)


def own_kernel(at, f_in, f_mid, f_out, force, solid, newton, inward, local, saved, offset):
    get = reader((f_out, at[OUT]), (f_mid, at[MID]), (f_in, at[IN]))
    keep(saved, collide(get, framed(force), solid[...], newton[...], offset, writer(1, into=(inward, 0), mid=(local, 0), out=(local, 9))))


def ghost_kernel(at, f_in, f_mid, f_out, cells, local, saved, offset):
    get = reader((f_out, at[OUT]), (f_mid, at[MID]), (f_in, at[IN]))
    keep(saved, collide(get, framed(cells, 18), cells[21], cells[22], offset, writer(1, into=(local, 0), mid=(local, 9))))


def cotangent_kernel(cotangent, after, outward, inward):
    odd = odd_device()
    for d in EVERY:
        value = cotangent[block_of(d[0], odd) + d[1] * 3 + d[2]]
        ref, start = ((outward, 0), (inward, 9), (inward, 0))[d[0]]
        ref[start + d[1] * 3 + d[2]] = moved(value, d[1], d[2], -1)


def turn_own_kernel(f_in, f_mid, f_out, force, solid, newton, m_in, m_mid, m_out, inward, final_mid, outward, local, push, offset):
    get = reader((f_out, 0), (f_mid, 0), (f_in, 0))
    saved = collide(get, framed(force), solid[...], newton[...], offset, writer(1, into=(inward, 0), mid=(final_mid, 0)))
    from_above = reader((m_out, 0), (m_mid, 9), (m_in, 0))
    keep(push, pull_back(from_above, saved, solid[...], writer(-1, out=(outward, 0), into=(local, 0), mid=(local, 9))))


def turn_ghost_kernel(f_in, f_mid, f_out, cells, m_in, m_mid, m_out, final_in, local, offset):
    get = reader((f_out, 9), (f_mid, 9), (f_in, 0))
    saved = collide(get, framed(cells, 18), cells[21], cells[22], offset, writer(1, into=(final_in, 0)))
    from_above = reader((m_out, 0), (m_mid, 9), (m_in, 0))
    pull_back(from_above, saved, cells[21], writer(-1, out=(local, 0), mid=(local, 9)))


def back_own_kernel(m_in, m_mid, m_out, saved, solid, push, outward, local, push_out):
    get = reader((m_out, 0), (m_mid, 9), (m_in, 0))
    terms = pull_back(get, saved_of(saved), solid[...], writer(-1, out=(outward, 0), into=(local, 0), mid=(local, 9)))
    for n in range(3):
        push_out[n] = push[n] + terms[n]


def back_ghost_kernel(m_in, m_mid, m_out, saved, cells, local):
    get = reader((m_out, 0), (m_mid, 9), (m_in, 0))
    pull_back(get, saved_of(saved), cells[21], writer(-1, out=(local, 0), mid=(local, 9)))


def last_kernel(m_in, m_mid, m_out, saved, solid, push, grad, grad_push):
    odd = odd_device()

    def emit(d, value):
        grad[block_of(d[0], odd) + d[1] * 3 + d[2]] = value()

    get = reader((m_out, 0), (m_mid, 9), (m_in, 0))
    terms = pull_back(get, saved_of(saved), solid[...], emit)
    grad_push[0] = facing(odd) * (push[0] + terms[0])
    grad_push[1] = push[1] + terms[1]
    grad_push[2] = push[2] + terms[2]


def final_kernel(f_in, f_mid, f_out, ratio):
    odd = odd_device()
    for a, ref in ((OUT, f_out), (MID, f_mid), (IN, f_in)):
        start = block_of(a, odd)
        for n in range(9):
            ratio[start + n] = ref[n]


def call(kernel, outs, *args, scratch=(27,), flops=4000000):
    plane = args[0].shape[1:]
    return pl.pallas_call(
        kernel,
        out_shape=[jax.ShapeDtypeStruct((n,) + plane, jnp.float32) for n in outs],
        scratch_shapes=[pltpu.VMEM((n,) + plane, jnp.float32) for n in scratch],
        compiler_params=pltpu.CompilerParams(vmem_limit_bytes=8 * 1024 * 1024),
        cost_estimate=pl.CostEstimate(flops=flops, bytes_accessed=1000000, transcendentals=0),
    )(*args)


def on_device(populations0, force, solid, newton, cotangent):
    devices = lax.axis_size(AXIS)
    rows = populations0.shape[2] // NZ

    def planes(x):
        return x.reshape(x.shape[:-2] + (rows, NZ))

    def partner(x):
        return lax.ppermute(x, AXIS, [(i, i ^ 1) for i in range(devices)])

    def inward_two(x):
        return lax.ppermute(x, AXIS, [(i, (i + 2 - 4 * (i % 2)) % devices) for i in range(devices)])

    def outward_one(x):
        return lax.ppermute(x, AXIS, [(i, (i - 1 + 2 * (i % 2)) % devices) for i in range(devices)])

    def outward_two(x):
        return inward_two(x)

    start, force, cotangent = planes(populations0), planes(force), planes(cotangent)
    solid, newton = solid.reshape(rows, NZ), newton.reshape(rows, NZ)
    cells = (force, solid, newton)

    inward, beside, saved0 = call(first_kernel, (9, 23, 4), start, *cells, scratch=(27, 27))
    far, near, ghost = inward_two(inward), partner(inward), outward_one(beside)
    inward, own1, saved1 = call(
        functools.partial(own_kernel, (0, 9, 0)), (9, 18, 4), ghost, beside, near, *cells
    )
    near1, far1 = partner(inward), inward_two(inward)
    ghost1, saved_ghost1 = call(functools.partial(ghost_kernel, (0, 9, 0)), (18, 4), far, ghost, beside, ghost)
    cot_out, cot_in = call(cotangent_kernel, (9, 18), cotangent, ghost1, scratch=(), flops=200000)
    inward, own2, saved2 = call(functools.partial(own_kernel, (0, 0, 0)), (9, 18, 4), ghost1, own1, near1, *cells)
    near2, far2 = partner(inward), inward_two(inward)
    cot_near, cot_far, cot_ghost = partner(cot_out), outward_two(cot_out), outward_one(cot_in)
    ghost2, saved_ghost2 = call(functools.partial(ghost_kernel, (9, 9, 0)), (18, 4), far1, ghost1, own1, ghost)
    last_in, last_mid, out3, own3, push = call(
        turn_own_kernel, (9, 9, 9, 18, 3), ghost2, own2, near2, *cells, cot_near, cot_in, cot_ghost
    )
    near3, far3 = partner(out3), outward_two(out3)
    last_ghost, ghost3 = call(
        turn_ghost_kernel, (9, 18), far2, ghost2, own2, ghost, cot_in, cot_ghost, cot_far
    )
    out2, own_b2, push = call(back_own_kernel, (9, 18, 3), near3, own3, ghost3, saved2, solid, push, scratch=(), flops=800000)
    near_b2, far_b2 = partner(out2), outward_two(out2)
    (ghost_b2,) = call(back_ghost_kernel, (18,), own3, ghost3, far3, saved_ghost2, ghost, scratch=(), flops=800000)
    out1, own_b1, push = call(back_own_kernel, (9, 18, 3), near_b2, own_b2, ghost_b2, saved1, solid, push, scratch=(), flops=800000)
    near_b1 = partner(out1)
    (ghost_b1,) = call(back_ghost_kernel, (18,), own_b2, ghost_b2, far_b2, saved_ghost1, ghost, scratch=(), flops=800000)
    grad, grad_push = call(last_kernel, (27, 3), near_b1, own_b1, ghost_b1, saved0, solid, push, scratch=(), flops=800000)
    last_near = partner(last_in)
    (ratio,) = call(final_kernel, (27,), last_ghost, last_mid, last_near, scratch=(), flops=200000)
    return (ratio.reshape(populations0.shape), grad.reshape(populations0.shape), grad_push.reshape(3, 1, rows * NZ))


def solution(mesh):
    return jax.shard_map(
        on_device,
        mesh=mesh,
        in_specs=(P(None, AXIS, None), P(None, AXIS, None), P(AXIS, None), P(AXIS, None), P(None, AXIS, None)),
        out_specs=(P(None, AXIS, None), P(None, AXIS, None), P(None, AXIS, None)),
        check_vma=False,
    )
```
